256 devices in a mesh: seq: 32 (over z, x), head: 2 (over core), batch: 4 (over y).
Axes of the slice: x: 4, y: 4, z: 8, core: 2. Of those that a mesh axis runs over, the one named last changes fastest.
Arguments:
- queries: bfloat16 [131072, 8, 256], P(('batch', 'seq'), 'head'), parts along dimension 0, may hold values from -6 to 6
- keys: bfloat16 [131072, 8, 256], P(('batch', 'seq'), 'head'), parts along dimension 0, may hold values from -0.375 to 0.375
- content_vectors: bfloat16 [131072, 8, 256], P(('batch', 'seq'), 'head'), parts along dimension 0, may hold values from -6 to 6
- decay_rate: float32 [8, 131072], P('head', ('batch', 'seq')), parts along dimension 1, may hold values from 0 to 3
- gate_pre: bfloat16 [131072, 2048], P(('batch', 'seq'), 'head'), parts along dimension 0, may hold values from -6 to 6
- norm_gain: float32 [2048], P('head'), may hold values from 0.1 to 1.9
- out_weight: bfloat16 [2048, 4096], P('head'), may hold values from -0.125 to 0.125
Outputs:
- layer_out: bfloat16 [131072, 4096], P(('batch', 'seq'), 'head'), parts along dimension 0
The draws below stay inside these ranges and needn't reach their ends.
There are 4 independent parts, one for each index of `batch`. The reference program is written for one: setup_inputs(seed, part) draws one part's arguments, and reference() takes and returns one part's arrays. A program takes and returns all parts, laid end to end along the dimension named above; an argument that names none is the same for every part. Nothing has to cross between parts.
All inputs are finite; a program needn't handle non-finite values.
Results may differ from the reference program's by a relative error of at most 0.013.
Values may be sent and summed in bfloat16 or wider, within the bound.
A program may use at most 128 MiB of HBM per device.

```python
import math
import jax
import jax.numpy as jnp
from jax import lax

D = 4096
HEADS = 8
DK = 256
VH = 256
TOK_DEV = 1024
TOKENS = 32768
N_SEQ = 32


def draw_decay_rate(key, part):
    keys_list = jax.random.split(jax.random.fold_in(key, 17), 7)
    ranking = jax.random.permutation(keys_list[0], HEADS)
    sluggish_tally = HEADS // 2
    is_slow = ranking < sluggish_tally
    fast_rate = jnp.exp(jax.random.uniform(keys_list[1], (HEADS,), jnp.float32, math.log(1.0 / 50.0), math.log(1.0 / 30.0)))
    slow_rate = jnp.exp(jax.random.uniform(keys_list[2], (HEADS,), jnp.float32, math.log(0.3 / TOKENS), math.log(0.6 / TOKENS)))
    baseline_decay = jnp.where(is_slow, slow_rate, fast_rate)
    segments = 2 * (TOKENS // TOK_DEV)
    gate_modulation = jnp.exp(jax.random.uniform(keys_list[3], (HEADS, segments), jnp.float32, -0.7, 0.7))
    gate_modulation = jnp.repeat(gate_modulation, TOK_DEV // 2, axis=1)
    noise_level = jax.random.uniform(keys_list[4], (HEADS, TOKENS), jnp.float32, 0.5, 1.5)
    destination_indices = jax.random.randint(keys_list[5], (HEADS, 3), 0, TOKENS)
    loss_values = jax.random.uniform(keys_list[6], (HEADS, 3), jnp.float32, -math.log(0.8), -math.log(0.5))
    token_positions = jnp.arange(TOKENS)
    spike_events = jnp.sum(jnp.where(token_positions[None, None, :] == destination_indices[:, :, None], loss_values[:, :, None], 0.0), axis=1)
    return (baseline_decay[:, None] * gate_modulation * noise_level + spike_events).astype(jnp.float32)


def level_of(rng, dims, shards, smallest, largest):
    loudness, own = 1.0, jax.random.fold_in(rng, 6)
    for position, blocks in shards:
        steps = jnp.exp(jax.random.uniform(jax.random.fold_in(own, position), (blocks,), jnp.float32, smallest / len(shards), largest / len(shards)))
        loudness = loudness * jnp.repeat(steps, dims[position] // blocks).reshape([-1 if axis == position else 1 for axis in range(len(dims))])
    return loudness


def bell_draw(stream_key, dims, scale, reach, pieces=(), dtype=jnp.bfloat16):
    array = jax.random.normal(stream_key, dims, jnp.float32) * scale
    if len(pieces) > 0:
        array = level_of(stream_key, dims, pieces, -0.22, 0.18) * array
    return jnp.clip(array, min=-reach, max=reach).astype(dtype)


def setup_inputs(seed: int = 0, part: int = 0) -> dict:
    seeds = jax.random.split(jax.random.key(seed), 8)
    own_keys = jax.random.split(jax.random.fold_in(seeds[7], part), 8)
    return {
        "queries": bell_draw(own_keys[0], (TOKENS, HEADS, DK), 1.0, 6.0, ((0, 32), (1, 2))),
        "keys": bell_draw(own_keys[1], (TOKENS, HEADS, DK), 0.0625, 0.375, ((0, 32), (1, 2))),
        "content_vectors": bell_draw(own_keys[2], (TOKENS, HEADS, VH), 1.0, 6.0, ((0, 32), (1, 2))),
        "decay_rate": draw_decay_rate(jax.random.fold_in(jax.random.fold_in(seeds[7], part), 71), part),
        "gate_pre": bell_draw(own_keys[4], (TOKENS, HEADS * VH), 1.0, 6.0, ((0, 32), (1, 2))),
        "norm_gain": jnp.clip(1.0 + 0.18 * jax.random.normal(seeds[5], (HEADS * VH,), jnp.float32), 0.1, 1.9),
        "out_weight": bell_draw(seeds[6], (HEADS * VH, D), (HEADS * VH) ** -0.5, 0.125, ((0, 2),)),
    }


def reference(queries, keys, content_vectors, decay_rate, gate_pre, norm_gain, out_weight):
    block_queries = queries.reshape(N_SEQ, TOK_DEV, HEADS, DK)
    block_keys = keys.reshape(N_SEQ, TOK_DEV, HEADS, DK)
    block_values = content_vectors.reshape(N_SEQ, TOK_DEV, HEADS, VH)
    block_rates = decay_rate.reshape(HEADS, N_SEQ, TOK_DEV).transpose(1, 0, 2)
    block_gates = gate_pre.reshape(N_SEQ, TOK_DEV, HEADS * VH)
    token_positions = jnp.arange(TOK_DEV)
    causal = token_positions[:, None] >= token_positions[None, :]

    def one_block(carried_state, inputs):
        current_query_rows, step_keys, present_content_vectors, step_rates, step_gates = inputs
        within = -jnp.cumsum(step_rates, axis=1)
        totals = within[:, -1]
        lookup_vectors_weighted = (jnp.exp(totals[None, :] - within.T)[:, :, None] * step_keys.astype(jnp.float32)).astype(jnp.bfloat16)
        segment_retained_matrix = jnp.einsum('gdj,gdl->djl', lookup_vectors_weighted.astype(jnp.float32), present_content_vectors.astype(jnp.float32))
        arriving_state = carried_state.astype(jnp.bfloat16)
        passed_forward = jnp.einsum('qaw,awi->qai', current_query_rows.astype(jnp.float32), arriving_state.astype(jnp.float32))
        passed_forward = passed_forward * jnp.exp(within.T)[:, :, None]
        scores = jnp.einsum('lhk,shk->hls', current_query_rows.astype(jnp.float32), step_keys.astype(jnp.float32))
        exponent = jnp.where(causal[None], within[:, :, None] - within[:, None, :], -jnp.inf)
        weights = (scores * jnp.exp(exponent)).astype(jnp.bfloat16)
        within_block = jnp.einsum('hls,shv->lhv', weights.astype(jnp.float32), present_content_vectors.astype(jnp.float32))
        retained = passed_forward + within_block
        center = lax.optimization_barrier(jnp.mean(retained, axis=2, keepdims=True))
        shifted = retained - center
        variance = lax.optimization_barrier(jnp.mean(shifted * shifted, axis=2, keepdims=True))
        normed = (shifted * lax.rsqrt(variance + 1e-06)).reshape(TOK_DEV, HEADS * VH)
        gated_rows = (normed * norm_gain * jax.nn.silu(step_gates.astype(jnp.float32))).astype(jnp.bfloat16)
        projected = jnp.dot(gated_rows, out_weight, preferred_element_type=jnp.float32).astype(jnp.bfloat16)
        next_state = jnp.exp(totals)[:, None, None] * carried_state + segment_retained_matrix
        return (next_state, projected)
    start_state = jnp.zeros((HEADS, DK, VH), jnp.float32)
    final_state, outputs = lax.scan(one_block, start_state, (block_queries, block_keys, block_values, block_rates, block_gates))
    return outputs.reshape(TOKENS, D)
```

```python
import jax
import jax.numpy as jnp
from jax import lax
from jax.experimental import pallas as pl
from jax.experimental.pallas import tpu as pltpu
from jax.sharding import PartitionSpec as P

NX, NZ = 4, 8
TOK, HL, DH = 1024, 4, 256
COLS = 2048
QR = DH // NX
PR, PC = 16, 128
TB = 256
BF, F32 = jnp.bfloat16, jnp.float32
MESH = pl.DeviceIdType.MESH


def kernel(
    q_hbm, k_hbm, v_hbm, d_hbm, gate_hbm, gain_ref, w_hbm, o_hbm,
    raw, kp, vp, qp, dec, gate, gfac, wcat, gcat, acc, ostage, within,
    perm, wrow, wcol, sb, xs, ab, zr, i0s, i0r, ins, inr,
    tsend, txr, etx, tzsend, tzr, etz,
    lsem, wsem, tx_s, tx_r, tz_s, tz_r, s1_s, s1_r, s2_s, s2_r, s3_s, s3_r, s4_s, s4_r,
    g_s, g_r, wr_s, wr_r, osem,
):
    seq = lax.axis_index("seq")
    core = lax.axis_index("head")
    x = lax.rem(seq, NX)
    z = lax.div(seq, NX)

    def x_peer(d):
        return lax.rem(x + d, NX)

    def z_peer(d):
        return lax.rem(z + d, NZ)

    def at_x(d):
        return {"seq": z * NX + x_peer(d)}

    def at_z(d):
        return {"seq": z_peer(d) * NX + x}

    partner = {"head": 1 - core}

    barrier = pltpu.get_barrier_semaphore()
    for d in range(1, NX):
        pl.semaphore_signal(barrier, inc=1, device_id=at_x(d), device_id_type=MESH)
    for d in range(1, NZ):
        pl.semaphore_signal(barrier, inc=1, device_id=at_z(d), device_id_type=MESH)
    pl.semaphore_signal(barrier, inc=1, device_id=partner, device_id_type=MESH)

    dcopy = pltpu.make_async_copy(d_hbm, dec, lsem.at[12])
    dcopy.start()
    ld = {}
    for n, (src, slot) in enumerate(((k_hbm, 0), (v_hbm, 1), (q_hbm, 2))):
        for c in range(4):
            rows = pl.ds(c * TB, TB)
            ld[n, c] = pltpu.make_async_copy(src.at[rows], raw.at[slot, rows], lsem.at[n * 4 + c])
    for n in (0, 1):
        for c in range(4):
            ld[n, c].start()
    gcopy = pltpu.make_async_copy(gate_hbm, gate, lsem.at[13])

    def remote(src, dst, ss, rs, dev):
        return pltpu.make_async_remote_copy(
            src_ref=src, dst_ref=dst, send_sem=ss, recv_sem=rs, device_id=dev, device_id_type=MESH
        )

    own_cols = pl.ds(pl.multiple_of(core * COLS, COLS), COLS)
    other_cols = pl.ds(pl.multiple_of((1 - core) * COLS, COLS), COLS)
    w_local, w_far = [], []
    for h in range(HL):
        rows = pl.ds(h * DH, DH)
        w_local.append(
            pltpu.make_async_copy(
                w_hbm.at[rows, own_cols], wcat.at[pl.ds(h * 2 * DH, DH)], wsem.at[h]
            )
        )
        w_far.append(
            remote(
                w_hbm.at[rows, other_cols], wcat.at[pl.ds(h * 2 * DH + DH, DH)],
                wr_s.at[h], wr_r.at[h], partner,
            )
        )

    ri = lax.broadcasted_iota(jnp.int32, (256, 256), 0)
    ci = lax.broadcasted_iota(jnp.int32, (256, 256), 1)
    perm[...] = jnp.where(ci == HL * (ri % 64) + ri // 64, 1.0, 0.0).astype(BF)

    ui = lax.broadcasted_iota(jnp.int32, (128, 256), 0)
    uj = lax.broadcasted_iota(jnp.int32, (128, 256), 1)
    upper = jnp.where(ui <= uj, 1.0, 0.0).astype(F32)
    dcopy.wait()
    stacked = jnp.concatenate([dec[:, c * 128:(c + 1) * 128] for c in range(8)], axis=0)
    sums = jnp.dot(stacked, upper, precision=lax.Precision.HIGHEST, preferred_element_type=F32)
    off = jnp.zeros((HL, 128), F32)
    parts = []
    for c in range(8):
        parts.append(-(off + sums[c * HL:(c + 1) * HL, :128]))
        off = off + sums[c * HL:(c + 1) * HL, 128:]
    w4 = jnp.concatenate(parts, axis=1)
    tot = -off
    tot8 = jnp.concatenate([tot] * 8, axis=1)
    ek = jnp.exp(tot8 - w4)
    eq = jnp.exp(w4)
    rows16 = jnp.concatenate([w4, ek, eq, eq], axis=0)
    wrow[...] = rows16
    wcol[...] = rows16.T
    tt = jnp.concatenate([tot, tot], axis=1)
    tsend[...] = jnp.concatenate([tt, tt], axis=0)
    txr[x] = tsend[...]

    pl.semaphore_wait(barrier, NX - 1 + NZ - 1 + 1)
    tx = [
        remote(tsend, txr.at[x], tx_s.at[d - 1], tx_r.at[d - 1], at_x(d)) for d in range(1, NX)
    ]
    for c in tx:
        c.start()

    def permute(n, dst):
        for c in range(4):
            ld[n, c].wait()
            for b in range(4):
                p0 = c * TB + b * 64
                r = jnp.dot(
                    perm[...], raw[n, p0:p0 + 64].reshape(256, 256), preferred_element_type=F32
                ).astype(BF)
                for h in range(HL):
                    dst[h, p0:p0 + 64, :] = r[h * 64:(h + 1) * 64]

    permute(0, kp)
    permute(1, vp)
    for c in range(4):
        ld[2, c].start()
    gcopy.start()
    for h in range(HL):
        w_local[h].start()
        w_far[h].start()

    s1 = {}
    for h in range(HL):
        scaled = (kp[h].astype(F32) * wcol[:, HL + h:HL + h + 1]).astype(BF)
        state = lax.dot_general(
            scaled, vp[h], (((0,), (0,)), ((), ())), preferred_element_type=F32
        ).astype(BF)
        for r in range(NX):
            sb[h, r] = state[r * QR:(r + 1) * QR]
        xs[h, x] = sb[h, x]
        for d in (1, 3, 2):
            s1[h, d] = remote(
                sb.at[h, x_peer(d)], xs.at[h, x], s1_s.at[h, d - 1], s1_r.at[h, d - 1], at_x(d)
            )
            s1[h, d].start()

    permute(2, qp)

    for c in tx:
        c.wait_recv()
    row_total = txr[0] + txr[1] + txr[2] + txr[3]
    tzsend[...] = row_total
    tzr[z] = row_total
    etx[...] = jnp.exp(txr[...])
    tz = [
        remote(tzsend, tzr.at[z], tz_s.at[d - 1], tz_r.at[d - 1], at_z(d)) for d in range(1, NZ)
    ]
    for c in tz:
        c.start()

    ti = lax.broadcasted_iota(jnp.int32, (TB, TB), 0)
    si = lax.broadcasted_iota(jnp.int32, (TB, TB), 1)

    def do_within(h):
        for tb in range(TOK // TB):
            t0 = tb * TB
            n = t0 + TB
            s = lax.dot_general(
                qp[h, t0:n, :], kp[h, :n, :], (((1,), (1,)), ((), ())), preferred_element_type=F32
            )
            wt = wcol[t0:n, h:h + 1]
            diag = jnp.where(ti >= si, wt - wrow[h:h + 1, t0:n], -jnp.inf)
            p = (s[:, t0:] * jnp.exp(diag)).astype(BF)
            if tb > 0:
                far = (s[:, :t0] * jnp.exp(wt - wrow[h:h + 1, :t0])).astype(BF)
                p = jnp.concatenate([far, p], axis=1)
            within[h, t0:n, :] = jnp.dot(p, vp[h, :n, :], preferred_element_type=F32)

    s2, s3, s4 = {}, {}, {}

    def stage_a(h):
        for d in range(1, NX):
            s1[h, d].wait_recv()
        a = xs[h, 0].astype(F32)
        for i in range(1, NX):
            a = a * etx[i, h:h + 1, :] + xs[h, i].astype(F32)
        a = a.astype(BF)
        for r in range(4):
            for c in range(2):
                ab[h, r + 4 * c] = a[r * PR:(r + 1) * PR, c * PC:(c + 1) * PC]
        zr[h, z] = ab[h, z]
        for d in (4, 3, 5, 2, 6, 1, 7):
            s2[h, d] = remote(
                ab.at[h, z_peer(d)], zr.at[h, z], s2_s.at[h, d - 1], s2_r.at[h, d - 1], at_z(d)
            )
            s2[h, d].start()

    def stage_z(h):
        for d in range(1, NZ):
            s2[h, d].wait_recv()
        run = zr[h, 0].astype(F32)
        i0s[h, 0] = jnp.zeros((PR, PC), BF)
        i0s[h, 1] = run.astype(BF)
        for i in range(1, NZ - 1):
            run = run * etz[i, h:h + 1, :PC] + zr[h, i].astype(F32)
            i0s[h, i + 1] = run.astype(BF)
        i0r[h, z] = i0s[h, z]
        for d in (4, 3, 5, 2, 6, 1, 7):
            s3[h, d] = remote(
                i0s.at[h, z_peer(d)], i0r.at[h, z], s3_s.at[h, d - 1], s3_r.at[h, d - 1], at_z(d)
            )
            s3[h, d].start()

    def stage_x(h):
        for d in range(1, NZ):
            s3[h, d].wait_recv()
        for r in range(4):
            for c in range(2):
                rows, cols = slice(r * PR, (r + 1) * PR), slice(c * PC, (c + 1) * PC)
                run = i0r[h, r + 4 * c].astype(F32)
                ins[h, 0, rows, cols] = run.astype(BF)
                for i in range(NX - 1):
                    run = run * etx[i, h:h + 1, cols] + xs[h, i, rows, cols].astype(F32)
                    ins[h, i + 1, rows, cols] = run.astype(BF)
        inr[h, x] = ins[h, x]
        for d in (2, 1, 3):
            s4[h, d] = remote(
                ins.at[h, x_peer(d)], inr.at[h, x], s4_s.at[h, d - 1], s4_r.at[h, d - 1], at_x(d)
            )
            s4[h, d].start()

    for h in range(HL):
        do_within(h)
        stage_a(h)

    for c in tz:
        c.wait_recv()
    etz[...] = jnp.exp(tzr[...])

    gcopy.wait()

    def gate_factor(h):
        cols = slice(h * DH, (h + 1) * DH)
        gp = gate[:, cols].astype(F32)
        gfac[:, cols] = gain_ref[:, cols] * (gp / (1.0 + jnp.exp(-gp)))

    for h in range(HL):
        gate_factor(h)
        stage_z(h)
    for h in range(HL):
        stage_x(h)

    gx = {}

    def finalize(h):
        for d in range(1, NX):
            s4[h, d].wait_recv()
        inc = inr[h].reshape(DH, DH)
        for tb in range(TOK // TB):
            rows = slice(tb * TB, (tb + 1) * TB)
            ret = jnp.dot(qp[h, rows, :], inc, preferred_element_type=F32)
            ret = ret * wcol[rows, 2 * HL + h:2 * HL + h + 1] + within[h, rows, :]
            center = jnp.mean(ret, axis=1, keepdims=True)
            shifted = ret - center
            variance = jnp.mean(shifted * shifted, axis=1, keepdims=True)
            normed = shifted * lax.rsqrt(variance + 1e-06)
            gcat[rows, h * 2 * DH:h * 2 * DH + DH] = (
                normed * gfac[rows, h * DH:(h + 1) * DH]
            ).astype(BF)
            rr = pl.ds(tb * TB, TB)
            gx[h, tb] = remote(
                gcat.at[rr, pl.ds(h * 2 * DH, DH)], gcat.at[rr, pl.ds(h * 2 * DH + DH, DH)],
                g_s.at[h, tb], g_r.at[h, tb], partner,
            )
            gx[h, tb].start()

    oc = []

    def project(h):
        w_local[h].wait()
        w_far[h].wait_recv()
        for tb in range(TOK // TB):
            gx[h, tb].wait_recv()
        depth = slice(h * 2 * DH, (h + 1) * 2 * DH)
        for j in range(COLS // 256):
            cols = slice(j * 256, (j + 1) * 256)
            part = jnp.dot(gcat[:, depth], wcat[depth, cols], preferred_element_type=F32)
            if h == 0:
                acc[:, cols] = part
            elif h < HL - 1:
                acc[:, cols] += part
            else:
                ostage[:, cols] = (acc[:, cols] + part).astype(BF)
                c = pltpu.make_async_copy(
                    ostage.at[:, pl.ds(j * 256, 256)], o_hbm.at[:, pl.ds(j * 256, 256)], osem.at[j]
                )
                c.start()
                oc.append(c)

    finalize(0)
    finalize(1)
    project(0)
    finalize(2)
    project(1)
    finalize(3)
    project(2)
    project(3)

    for group in (s1, s2, s3, s4, gx):
        for c in group.values():
            c.wait_send()
    for group in (tx, tz, w_far):
        for c in group:
            c.wait_send()
    for c in oc:
        c.wait()


def on_device(queries, keys, content_vectors, decay_rate, gate_pre, norm_gain, out_weight):
    hbm = pl.BlockSpec(memory_space=pl.ANY)
    vmem = pl.BlockSpec(memory_space=pltpu.VMEM)
    dma = pltpu.SemaphoreType.DMA
    scratch = [
        pltpu.VMEM((3, TOK, HL, DH), BF),
        pltpu.VMEM((HL, TOK, DH), BF),
        pltpu.VMEM((HL, TOK, DH), BF),
        pltpu.VMEM((HL, TOK, DH), BF),
        pltpu.VMEM((HL, TOK), F32),
        pltpu.VMEM((TOK, HL * DH), BF),
        pltpu.VMEM((TOK, HL * DH), F32),
        pltpu.VMEM((2 * HL * DH, COLS), BF),
        pltpu.VMEM((TOK, 2 * HL * DH), BF),
        pltpu.VMEM((TOK, COLS), F32),
        pltpu.VMEM((TOK, COLS), BF),
        pltpu.VMEM((HL, TOK, DH), F32),
        pltpu.VMEM((256, 256), BF),
        pltpu.VMEM((4 * HL, TOK), F32),
        pltpu.VMEM((TOK, 4 * HL), F32),
        pltpu.VMEM((HL, NX, QR, DH), BF),
        pltpu.VMEM((HL, NX, QR, DH), BF),
        pltpu.VMEM((HL, NZ, PR, PC), BF),
        pltpu.VMEM((HL, NZ, PR, PC), BF),
        pltpu.VMEM((HL, NZ, PR, PC), BF),
        pltpu.VMEM((HL, NZ, PR, PC), BF),
        pltpu.VMEM((HL, NX, QR, DH), BF),
        pltpu.VMEM((HL, NX, QR, DH), BF),
        pltpu.VMEM((8, DH), F32),
        pltpu.VMEM((NX, 8, DH), F32),
        pltpu.VMEM((NX, 8, DH), F32),
        pltpu.VMEM((8, DH), F32),
        pltpu.VMEM((NZ, 8, DH), F32),
        pltpu.VMEM((NZ, 8, DH), F32),
        dma((14,)), dma((HL,)),
        dma((NX - 1,)), dma((NX - 1,)), dma((NZ - 1,)), dma((NZ - 1,)),
        dma((HL, NX - 1)), dma((HL, NX - 1)), dma((HL, NZ - 1)), dma((HL, NZ - 1)),
        dma((HL, NZ - 1)), dma((HL, NZ - 1)), dma((HL, NX - 1)), dma((HL, NX - 1)),
        dma((HL, TOK // TB)), dma((HL, TOK // TB)), dma((HL,)), dma((HL,)), dma((COLS // 256,)),
    ]
    return pl.pallas_call(
        kernel,
        out_shape=jax.ShapeDtypeStruct((TOK, COLS), BF),
        in_specs=[hbm, hbm, hbm, hbm, hbm, vmem, hbm],
        out_specs=hbm,
        scratch_shapes=scratch,
        compiler_params=pltpu.CompilerParams(
            collective_id=0, has_side_effects=True, vmem_limit_bytes=62 * 1024 * 1024
        ),
        name="retention",
    )(queries, keys, content_vectors, decay_rate, gate_pre, norm_gain.reshape(1, -1), out_weight)


def solution(mesh):
    in_specs = (
        P(("batch", "seq"), "head", None),
        P(("batch", "seq"), "head", None),
        P(("batch", "seq"), "head", None),
        P("head", ("batch", "seq")),
        P(("batch", "seq"), "head"),
        P("head"),
        P("head", None),
    )
    out_specs = P(("batch", "seq"), "head")
    return jax.shard_map(
        on_device, mesh=mesh, in_specs=in_specs, out_specs=out_specs, check_vma=False
    )
```

```python
import jax
import jax.numpy as jnp
from jax import lax
from jax.experimental import pallas as pl
from jax.experimental.pallas import tpu as pltpu
from jax.sharding import PartitionSpec as P

NX, NZ = 4, 8
TOK, HL, DH = 1024, 4, 256
COLS = 2048
QR = DH // NX
PR, PC = 16, 128
TB = 256
BF, F32 = jnp.bfloat16, jnp.float32
MESH = pl.DeviceIdType.MESH
SC = jax.named_scope
VMEM_MIB = 56


def kernel(
    q_hbm, k_hbm, v_hbm, d_hbm, gate_hbm, gain_ref, w_hbm, o_ref,
    raw, kp, ks, vp, qp, dec, gate, gfac, wcat, gcat, acc, within,
    perm, wrow, wcol, sb, xs, ab, zr, i0s, i0r, ins, inr,
    tsend, txr, etx, tzsend, tzr, etz,
    lsem, tx_s, tx_r, tz_s, tz_r, s1_s, s1_r, s2_s, s2_r, s3_s, s3_r, s4_s, s4_r,
    g_s, g_r, wr_s, wr_r,
):
    seq = lax.axis_index("seq")
    core = lax.axis_index("head")
    x = lax.rem(seq, NX)
    z = lax.div(seq, NX)

    def x_peer(d):
        return lax.rem(x + d, NX)

    def z_peer(d):
        return lax.rem(z + d, NZ)

    def at_x(d):
        return {"seq": z * NX + x_peer(d)}

    def at_z(d):
        return {"seq": z_peer(d) * NX + x}

    partner = {"head": 1 - core}

    barrier = pltpu.get_barrier_semaphore()
    for d in range(1, NX):
        pl.semaphore_signal(barrier, inc=1, device_id=at_x(d), device_id_type=MESH)
    for d in range(1, NZ):
        pl.semaphore_signal(barrier, inc=1, device_id=at_z(d), device_id_type=MESH)
    pl.semaphore_signal(barrier, inc=1, device_id=partner, device_id_type=MESH)

    dcopy = pltpu.make_async_copy(d_hbm, dec, lsem.at[0])
    dcopy.start()
    loads = []
    for n, src in enumerate((k_hbm, v_hbm, q_hbm)):
        for c in range(4):
            rows = pl.ds(c * TB, TB)
            loads.append(pltpu.make_async_copy(src.at[rows], raw.at[n, rows], lsem.at[1 + n]))
    for c in loads[:8]:
        c.start()
    gcopy = pltpu.make_async_copy(gate_hbm, gate, lsem.at[4])

    def arrived(ref, sem):
        pltpu.make_async_copy(ref, ref, sem).wait()

    def remote(src, dst, ss, rs, dev):
        return pltpu.make_async_remote_copy(
            src_ref=src, dst_ref=dst, send_sem=ss, recv_sem=rs, device_id=dev, device_id_type=MESH
        )

    own_cols = pl.ds(pl.multiple_of(core * COLS, COLS), COLS)
    other_cols = pl.ds(pl.multiple_of((1 - core) * COLS, COLS), COLS)
    w_local, w_far = [], []
    for h in range(HL):
        rows = pl.ds(h * DH, DH)
        w_local.append(
            pltpu.make_async_copy(
                w_hbm.at[rows, own_cols], wcat.at[pl.ds(h * 2 * DH, DH)], lsem.at[5]
            )
        )
        w_far.append(
            remote(
                w_hbm.at[rows, other_cols], wcat.at[pl.ds(h * 2 * DH + DH, DH)],
                wr_s.at[0], wr_r.at[h], partner,
            )
        )

    ri = lax.broadcasted_iota(jnp.int32, (256, 256), 0)
    ci = lax.broadcasted_iota(jnp.int32, (256, 256), 1)
    perm[...] = jnp.where(ci == HL * (ri % 64) + ri // 64, 1.0, 0.0).astype(BF)

    ui = lax.broadcasted_iota(jnp.int32, (128, 256), 0)
    uj = lax.broadcasted_iota(jnp.int32, (128, 256), 1)
    upper = jnp.where(ui <= uj, 1.0, 0.0).astype(F32)
    dcopy.wait()
    stacked = jnp.concatenate([dec[:, c * 128:(c + 1) * 128] for c in range(8)], axis=0)
    sums = jnp.dot(stacked, upper, precision=lax.Precision.HIGHEST, preferred_element_type=F32)
    off = jnp.zeros((HL, 128), F32)
    parts = []
    for c in range(8):
        parts.append(-(off + sums[c * HL:(c + 1) * HL, :128]))
        off = off + sums[c * HL:(c + 1) * HL, 128:]
    w4 = jnp.concatenate(parts, axis=1)
    tot = -off
    tot8 = jnp.concatenate([tot] * 8, axis=1)
    ek = jnp.exp(tot8 - w4)
    eq = jnp.exp(w4)
    rows16 = jnp.concatenate([w4, ek, eq, eq], axis=0)
    wrow[...] = rows16
    wcol[...] = rows16.T
    tt = jnp.concatenate([tot, tot], axis=1)
    tsend[...] = jnp.concatenate([tt, tt], axis=0)
    txr[x] = tsend[...]

    def permute(n, dst, scaled=None):
        arrived(raw.at[n], lsem.at[1 + n])
        for b in range(TOK // 64):
            p0 = b * 64
            r = jnp.dot(
                perm[...], raw[n, p0:p0 + 64].reshape(256, 256), preferred_element_type=F32
            )
            for h in range(HL):
                rh = r[h * 64:(h + 1) * 64]
                dst[h, p0:p0 + 64, :] = rh.astype(BF)
                if scaled is not None:
                    scaled[h, p0:p0 + 64, :] = (rh * wcol[p0:p0 + 64, HL + h:HL + h + 1]).astype(BF)

    with SC("permk"):
        permute(0, kp, ks)
    with SC("permv"):
        permute(1, vp)
    for c in loads[8:]:
        c.start()
    gcopy.start()

    def state(h):
        value = lax.dot_general(
            ks[h], vp[h], (((0,), (0,)), ((), ())), preferred_element_type=F32
        ).astype(BF)
        for r in range(NX):
            sb[h, r] = value[r * QR:(r + 1) * QR]
        xs[h, x] = sb[h, x]

    def send_state(h):
        for d in (1, 3, 2):
            remote(sb.at[h, x_peer(d)], xs.at[h, x], s1_s.at[0], s1_r.at[h], at_x(d)).start()

    with SC("state0"):
        state(0)
    with SC("barrier"):
        pl.semaphore_wait(barrier, NX - 1 + NZ - 1 + 1)
    for d in range(1, NX):
        remote(tsend, txr.at[x], tx_s.at[0], tx_r.at[0], at_x(d)).start()
    send_state(0)
    with SC("state123"):
        for h in range(1, HL):
            state(h)
            send_state(h)
    with SC("permq"):
        permute(2, qp)
    for h in range(HL):
        w_local[h].start()
    w_far[0].start()

    def row_totals():
        with SC("txwait"):
            arrived(txr.at[pl.ds(0, NX - 1)], tx_r.at[0])
        row_total = txr[0] + txr[1] + txr[2] + txr[3]
        tzsend[...] = row_total
        tzr[z] = row_total
        etx[...] = jnp.exp(txr[...])
        for d in range(1, NZ):
            remote(tzsend, tzr.at[z], tz_s.at[0], tz_r.at[0], at_z(d)).start()

    ti = lax.broadcasted_iota(jnp.int32, (TB, TB), 0)
    si = lax.broadcasted_iota(jnp.int32, (TB, TB), 1)

    def do_within(h):
        for tb in range(TOK // TB):
            t0 = tb * TB
            n = t0 + TB
            s = lax.dot_general(
                qp[h, t0:n, :], kp[h, :n, :], (((1,), (1,)), ((), ())), preferred_element_type=F32
            )
            wt = wcol[t0:n, h:h + 1]
            diag = jnp.where(ti >= si, wt - wrow[h:h + 1, t0:n], -jnp.inf)
            p = (s[:, t0:] * jnp.exp(diag)).astype(BF)
            if tb > 0:
                far = (s[:, :t0] * jnp.exp(wt - wrow[h:h + 1, :t0])).astype(BF)
                p = jnp.concatenate([far, p], axis=1)
            within[h, t0:n, :] = jnp.dot(p, vp[h, :n, :], preferred_element_type=F32)

    def stage_a(h):
        with SC(f"Await{h}"):
            arrived(xs.at[h, pl.ds(0, NX - 1)], s1_r.at[h])
        a = xs[h, 0].astype(F32)
        for i in range(1, NX):
            a = a * etx[i, h:h + 1, :] + xs[h, i].astype(F32)
        a = a.astype(BF)
        for r in range(4):
            for c in range(2):
                ab[h, r + 4 * c] = a[r * PR:(r + 1) * PR, c * PC:(c + 1) * PC]
        zr[h, z] = ab[h, z]
        for d in (4, 3, 5, 2, 6, 1, 7):
            remote(ab.at[h, z_peer(d)], zr.at[h, z], s2_s.at[0], s2_r.at[h], at_z(d)).start()

    def stage_z(h):
        with SC(f"Zwait{h}"):
            arrived(zr.at[h, pl.ds(0, NZ - 1)], s2_r.at[h])
        run = zr[h, 0].astype(F32)
        i0s[h, 0] = jnp.zeros((PR, PC), BF)
        i0s[h, 1] = run.astype(BF)
        for i in range(1, NZ - 1):
            run = run * etz[i, h:h + 1, :PC] + zr[h, i].astype(F32)
            i0s[h, i + 1] = run.astype(BF)
        i0r[h, z] = i0s[h, z]
        for d in (4, 3, 5, 2, 6, 1, 7):
            remote(i0s.at[h, z_peer(d)], i0r.at[h, z], s3_s.at[0], s3_r.at[h], at_z(d)).start()

    def stage_x(h):
        with SC(f"Xwait{h}"):
            arrived(i0r.at[h, pl.ds(0, NZ - 1)], s3_r.at[h])
        for r in range(4):
            for c in range(2):
                rows, cols = slice(r * PR, (r + 1) * PR), slice(c * PC, (c + 1) * PC)
                run = i0r[h, r + 4 * c].astype(F32)
                ins[h, 0, rows, cols] = run.astype(BF)
                for i in range(NX - 1):
                    run = run * etx[i, h:h + 1, cols] + xs[h, i, rows, cols].astype(F32)
                    ins[h, i + 1, rows, cols] = run.astype(BF)
        inr[h, x] = ins[h, x]
        for d in (2, 1, 3):
            remote(ins.at[h, x_peer(d)], inr.at[h, x], s4_s.at[0], s4_r.at[h], at_x(d)).start()

    for h in range(HL):
        with SC(f"within{h}"):
            do_within(h)
        if h == 0:
            row_totals()
        stage_a(h)
        if h == 0:
            w_far[1].start()

    with SC("tzwait"):
        arrived(tzr.at[pl.ds(0, NZ - 1)], tz_r.at[0])
    etz[...] = jnp.exp(tzr[...])

    gcopy.wait()

    def gate_factor(h):
        cols = slice(h * DH, (h + 1) * DH)
        gp = gate[:, cols].astype(F32)
        gfac[:, cols] = gain_ref[:, cols] * (gp / (1.0 + jnp.exp(-gp)))

    for h in range(HL):
        with SC(f"gate{h}"):
            gate_factor(h)
        stage_z(h)
        if h == 0:
            w_far[2].start()
    for h in range(HL):
        stage_x(h)
        if h == 0:
            w_far[3].start()

    def incoming_wait(h):
        with SC(f"Fwait{h}"):
            arrived(inr.at[h, pl.ds(0, NX - 1)], s4_r.at[h])

    def finalize(h, tb):
        rows = slice(tb * TB, (tb + 1) * TB)
        inc = inr[h].reshape(DH, DH)
        ret = jnp.dot(qp[h, rows, :], inc, preferred_element_type=F32)
        ret = ret * wcol[rows, 2 * HL + h:2 * HL + h + 1] + within[h, rows, :]
        center = jnp.mean(ret, axis=1, keepdims=True)
        shifted = ret - center
        variance = jnp.mean(shifted * shifted, axis=1, keepdims=True)
        normed = shifted * lax.rsqrt(variance + 1e-06)
        gcat[rows, h * 2 * DH:h * 2 * DH + DH] = (
            normed * gfac[rows, h * DH:(h + 1) * DH]
        ).astype(BF)

    def exchange(h):
        remote(
            gcat.at[:, pl.ds(h * 2 * DH, DH)], gcat.at[:, pl.ds(h * 2 * DH + DH, DH)],
            g_s.at[0], g_r.at[h], partner,
        ).start()

    def partner_wait(h):
        with SC(f"pwait{h}"):
            w_far[h].wait_recv()
            arrived(gcat.at[:, pl.ds(h * 2 * DH + DH, DH)], g_r.at[h])

    def project(n, j):
        depth = slice(max(2 * n - 1, 0) * DH, min(2 * n + 1, 2 * HL) * DH)
        cols = slice(j * 256, (j + 1) * 256)
        part = jnp.dot(gcat[:, depth], wcat[depth, cols], preferred_element_type=F32)
        if n == 0:
            acc[:, cols] = part
        elif n < HL:
            acc[:, cols] += part
        else:
            o_ref[:, cols] = (acc[:, cols] + part).astype(BF)

    blocks = TOK // TB
    incoming_wait(0)
    with SC("finalize0"):
        for tb in range(blocks):
            finalize(0, tb)
    exchange(0)
    arrived(wcat.at[pl.ds(0, HL * DH)], lsem.at[5])
    for n in range(HL + 1):
        if n > 0:
            partner_wait(n - 1)
        if n + 1 < HL:
            incoming_wait(n + 1)
        with SC(f"project{n}"):
            for j in range(COLS // 256):
                project(n, j)
                if n + 1 < HL and j % 2 == 1:
                    finalize(n + 1, j // 2)
        if n + 1 < HL:
            exchange(n + 1)

    with SC("sendwait"):
        arrived(sb.at[:, pl.ds(0, NX - 1)], s1_s.at[0])
        arrived(ab.at[:, pl.ds(0, NZ - 1)], s2_s.at[0])
        arrived(i0s.at[:, pl.ds(0, NZ - 1)], s3_s.at[0])
        arrived(ins.at[:, pl.ds(0, NX - 1)], s4_s.at[0])
        arrived(txr.at[pl.ds(0, NX - 1)], tx_s.at[0])
        arrived(tzr.at[pl.ds(0, NZ - 1)], tz_s.at[0])
        arrived(wcat.at[pl.ds(0, HL * DH)], wr_s.at[0])
        arrived(gcat.at[:, pl.ds(0, HL * DH)], g_s.at[0])


def on_device(queries, keys, content_vectors, decay_rate, gate_pre, norm_gain, out_weight):
    hbm = pl.BlockSpec(memory_space=pl.ANY)
    vmem = pl.BlockSpec(memory_space=pltpu.VMEM)
    dma = pltpu.SemaphoreType.DMA
    scratch = [
        pltpu.VMEM((3, TOK, HL, DH), BF),
        pltpu.VMEM((HL, TOK, DH), BF),
        pltpu.VMEM((HL, TOK, DH), BF),
        pltpu.VMEM((HL, TOK, DH), BF),
        pltpu.VMEM((HL, TOK, DH), BF),
        pltpu.VMEM((HL, TOK), F32),
        pltpu.VMEM((TOK, HL * DH), BF),
        pltpu.VMEM((TOK, HL * DH), F32),
        pltpu.VMEM((2 * HL * DH, COLS), BF),
        pltpu.VMEM((TOK, 2 * HL * DH), BF),
        pltpu.VMEM((TOK, COLS), F32),
        pltpu.VMEM((HL, TOK, DH), F32),
        pltpu.VMEM((256, 256), BF),
        pltpu.VMEM((4 * HL, TOK), F32),
        pltpu.VMEM((TOK, 4 * HL), F32),
        pltpu.VMEM((HL, NX, QR, DH), BF),
        pltpu.VMEM((HL, NX, QR, DH), BF),
        pltpu.VMEM((HL, NZ, PR, PC), BF),
        pltpu.VMEM((HL, NZ, PR, PC), BF),
        pltpu.VMEM((HL, NZ, PR, PC), BF),
        pltpu.VMEM((HL, NZ, PR, PC), BF),
        pltpu.VMEM((HL, NX, QR, DH), BF),
        pltpu.VMEM((HL, NX, QR, DH), BF),
        pltpu.VMEM((8, DH), F32),
        pltpu.VMEM((NX, 8, DH), F32),
        pltpu.VMEM((NX, 8, DH), F32),
        pltpu.VMEM((8, DH), F32),
        pltpu.VMEM((NZ, 8, DH), F32),
        pltpu.VMEM((NZ, 8, DH), F32),
        dma((6,)), dma((1,)), dma((1,)), dma((1,)), dma((1,)),
        dma((1,)), dma((HL,)), dma((1,)), dma((HL,)),
        dma((1,)), dma((HL,)), dma((1,)), dma((HL,)),
        dma((1,)), dma((HL,)), dma((1,)), dma((HL,)),
    ]
    return pl.pallas_call(
        kernel,
        out_shape=pltpu.VMEM((TOK, COLS), BF),
        in_specs=[hbm, hbm, hbm, hbm, hbm, vmem, hbm],
        out_specs=vmem,
        scratch_shapes=scratch,
        compiler_params=pltpu.CompilerParams(
            collective_id=0, has_side_effects=True, vmem_limit_bytes=VMEM_MIB * 1024 * 1024
        ),
        name="retention",
    )(queries, keys, content_vectors, decay_rate, gate_pre, norm_gain.reshape(1, -1), out_weight)


def solution(mesh):
    in_specs = (
        P(("batch", "seq"), "head", None),
        P(("batch", "seq"), "head", None),
        P(("batch", "seq"), "head", None),
        P("head", ("batch", "seq")),
        P(("batch", "seq"), "head"),
        P("head"),
        P("head", None),
    )
    out_specs = P(("batch", "seq"), "head")
    return jax.shard_map(
        on_device, mesh=mesh, in_specs=in_specs, out_specs=out_specs, check_vma=False
    )
```
